32 devices in a mesh: tp: 2 (over x), dp: 4 (over y, core), rep: 4 (over z).
Axes of the slice: x: 2, y: 2, z: 4, core: 2. Of those that a mesh axis runs over, the one named last changes fastest.
Arguments:
- prompts: bfloat16 [12288, 8192], P(('dp', 'rep'), 'tp'), may hold values from -6 to 6
- frozen_projection_weight: bfloat16 [2, 8192, 2048], P(None, ('dp', 'rep'), 'tp'), may hold values from -5 to 5
- lowrank_down_factor: bfloat16 [2, 8192, 64], P(None, ('dp', 'rep')), may hold values from -0.119628906 to 0.119628906
- lowrank_up_factor: bfloat16 [2, 64, 2048], P(None, None, 'tp'), may hold values from -0.59765625 to 0.59765625
- magnitude: float32 [2, 2048], P(None, 'tp'), may hold values from 0.5 to 2
Outputs:
- key_values: bfloat16 [2, 12288, 2048], P(None, ('dp', 'rep'), 'tp')
The draws below stay inside these ranges and needn't reach their ends.
All inputs are finite; a program needn't handle non-finite values.
Results may differ from the reference program's by a relative error of at most 0.0049.
Values may be sent and summed in bfloat16 or wider, within the bound.
A program may use at most 128 MiB of HBM per device.

```python
import math
import jax
import jax.numpy as jnp
from jax import lax

MODEL_WIDTH = 8192
LOWRANK_SIZE = 64
LAYER_COUNT = 2
PROJECTION_COLUMNS = 2048
TOKENS = 12288


def draw_frozen_projection_weight(key, part):
    streams = jax.random.split(jax.random.fold_in(key, 17), 3)
    position = jnp.arange(MODEL_WIDTH, dtype=jnp.float32)[None, :, None] / MODEL_WIDTH
    row_rough = jnp.exp(jax.random.uniform(streams[1], (LAYER_COUNT, MODEL_WIDTH, 1), jnp.float32, -1.2, 1.2))
    col_rough = jnp.exp(jax.random.uniform(streams[2], (LAYER_COUNT, 1, PROJECTION_COLUMNS), jnp.float32, -1.2, 1.2))
    noise = jnp.clip(jax.random.normal(streams[0], (LAYER_COUNT, MODEL_WIDTH, PROJECTION_COLUMNS), jnp.float32), -4.0, 4.0)
    ramp = jnp.sqrt(1.0 + 2.0 * position)
    values = noise * row_rough * col_rough * ramp / math.sqrt(MODEL_WIDTH)
    return values.astype(jnp.bfloat16)


def steps_of(key, extent, cuts, low, top_value):
    gain = 1.0
    for dim, shards_of in cuts:
        draws = jax.random.uniform(jax.random.fold_in(jax.random.fold_in(key, 6), dim), (shards_of,), jnp.float32, low / len(cuts), top_value / len(cuts))
        gain = gain * jnp.repeat(jnp.exp(draws), extent[dim] // shards_of).reshape((-1,) + (1,) * (len(extent) - 1 - dim))
    return gain


def gaussian(rng, shape, deviation, reach, shards=(), held_as=jnp.bfloat16):
    values = jax.random.normal(rng, shape, jnp.float32) * deviation
    if len(shards) > 0:
        values = steps_of(rng, shape, shards, -0.22, 0.18) * values
    return jnp.clip(values, min=-reach, max=reach).astype(held_as)


def setup_inputs(seed: int = 0) -> dict:
    keys = jax.random.split(jax.random.key(seed), 6)
    return {
        "prompts": gaussian(keys[0], (TOKENS, MODEL_WIDTH), 1.0, 6.0, ((0, 16), (1, 2))),
        "frozen_projection_weight": draw_frozen_projection_weight(jax.random.fold_in(keys[5], 71), 0),
        "lowrank_down_factor": gaussian(keys[2], (LAYER_COUNT, MODEL_WIDTH, LOWRANK_SIZE), 0.02, 0.119628906, ((1, 16),)),
        "lowrank_up_factor": gaussian(keys[3], (LAYER_COUNT, LOWRANK_SIZE, PROJECTION_COLUMNS), 0.1, 0.59765625, ((2, 2),)),
        "magnitude": jnp.clip(jnp.exp(math.log(2.0) - 1.3862944 * jax.random.uniform(keys[4], (LAYER_COUNT, PROJECTION_COLUMNS), jnp.float32) ** steps_of(keys[4], (LAYER_COUNT, PROJECTION_COLUMNS), ((1, 2),), -0.2, 0.2)), 0.5, 2.0),
    }


epsilon = 1e-06

def reference(prompts, frozen_projection_weight, lowrank_down_factor, lowrank_up_factor, magnitude):
    outputs = []
    for current_layer_index in range(LAYER_COUNT):
        combined_weight = frozen_projection_weight[current_layer_index].astype(jnp.float32) + jnp.dot(lowrank_down_factor[current_layer_index], lowrank_up_factor[current_layer_index], preferred_element_type=jnp.float32)
        norms = jnp.sqrt(lax.optimization_barrier(jnp.sum(combined_weight * combined_weight, axis=0)) + epsilon)
        factor = magnitude[current_layer_index] / norms
        prefilled_key_values = (combined_weight * factor).astype(jnp.bfloat16)
        outputs.append(jnp.dot(prompts, prefilled_key_values, preferred_element_type=jnp.float32).astype(jnp.bfloat16))
    return jnp.stack(outputs)
```

```python
import functools

import jax
import jax.numpy as jnp
from jax import lax
from jax.experimental import pallas as pl
from jax.experimental.pallas import tpu as pltpu
from jax.sharding import PartitionSpec as P

epsilon = 1e-06
MESH = pl.DeviceIdType.MESH


def kernel(
    sizes, prompts_ref, weight_ref, down_ref, up_ref, magnitude_ref, out_ref,
    wbuf, pbuf, dbuf, ubuf, acc, squares,
    arrive, zup, zdown, ysend, csend, psend, parrive, load_p, load_w, load_f,
):
    tp_size, dp_size, rep_size = sizes
    y_size = dp_size // 2
    layers, rows, columns = weight_ref.shape
    tokens = prompts_ref.shape[0]
    half = rows // 2
    count = 2 * layers
    groups = dp_size // tp_size
    x = lax.axis_index("tp")
    d = lax.axis_index("dp")
    z = lax.axis_index("rep")
    y, c = d // 2, lax.rem(d, 2)
    partner = {"tp": x, "dp": d + 1 - 2 * c, "rep": z}
    last = rep_size - 1
    middle = (z > 0) & (z < last)

    def column(o):
        return lax.rem(y + o, y_size)

    def block(yy, cc, zz):
        return (yy * 2 + cc) * rep_size + zz

    def piece(b, k):
        start = pl.multiple_of(k // layers * half, half)
        return wbuf.at[b, lax.rem(k, layers), pl.ds(start, half), :]

    def ranked(at):
        longer = -1 if at > last - at else 1
        return sorted(range(rep_size), key=lambda k: (abs(k - at), -longer * (k - at)))

    table = [ranked(at) for at in range(rep_size)]

    def plane(i):
        value = jnp.int32(0)
        for at in range(rep_size):
            for step in range(rep_size):
                value = jnp.where((z == at) & (i == step), jnp.int32(table[at][step]), value)
        return value

    def doubled(zz, k):
        return ((zz == 0) | (zz == last)) & (k >= layers)

    def y_device(o):
        return {"tp": x, "dp": column(o) * 2 + c, "rep": z}

    def z_device(step):
        return {"tp": x, "dp": d, "rep": z + step}

    def remote(ref, send_sem, recv_sem, device):
        return pltpu.make_async_remote_copy(
            src_ref=ref, dst_ref=ref, send_sem=send_sem, recv_sem=recv_sem,
            device_id=device, device_id_type=MESH,
        )

    def wait_piece(b, k):
        remote(piece(b, k), csend.at[0], arrive.at[b * count + k], partner).wait_recv()

    def copies(o, zz, k, act):
        yy = column(o)
        b = block(yy, c, zz)
        ref, landed = piece(b, k), arrive.at[b * count + k]
        at = (yy * rep_size + zz) * count + k
        onz = doubled(zz, k)
        along = onz if o > 0 else (z >= 0)

        @pl.when(along & (zz >= z) & (z > 0))
        def _():
            act(remote(ref, zdown.at[at], landed, z_device(-1)))

        @pl.when(along & (zz <= z) & (z < last))
        def _():
            act(remote(ref, zup.at[at], landed, z_device(1)))

        if o == 0:
            for p in range(1, y_size):
                @pl.when((zz == z) | jnp.logical_not(onz))
                def _(p=p):
                    act(remote(ref, ysend.at[((p - 1) * rep_size + zz) * count + k], landed, y_device(p)))

        act(remote(ref, csend.at[at], landed, partner))

    def forward(o, zz, k):
        copies(o, zz, k, lambda copy: copy.start())

    def duty(o, zz, k):
        wait_piece(block(column(o), c, zz), k)
        forward(o, zz, k)

    me = block(y, c, z)

    def load_weight(k):
        start = k // layers * half
        return pltpu.make_async_copy(
            weight_ref.at[k % layers, pl.ds(start, half), :], piece(me, jnp.int32(k)), load_w.at[k]
        )

    load_down = pltpu.make_async_copy(down_ref, dbuf, load_f.at[0])
    load_up = pltpu.make_async_copy(up_ref, ubuf, load_f.at[1])
    load_down.start()
    load_up.start()
    for k in range(count):
        load_weight(k).start()

    own_chunks = []
    for i in range(rep_size):
        for g in range(groups):
            zz = plane(i)
            own_chunks.append((g * rep_size + zz, x * groups * rep_size + g * rep_size + zz))

    def load_chunk(j, b):
        start = pl.multiple_of(j * rows, rows)
        return pltpu.make_async_copy(prompts_ref.at[:, pl.ds(start, rows)], pbuf.at[b], load_p.at[b])

    for j, b in own_chunks:
        load_chunk(j, b).start()

    barrier = pltpu.get_barrier_semaphore()
    pl.semaphore_signal(barrier, 1, device_id=partner, device_id_type=MESH)
    for o in range(1, y_size):
        pl.semaphore_signal(barrier, 1, device_id=y_device(o), device_id_type=MESH)
    for o in range(1, tp_size):
        pl.semaphore_signal(
            barrier, 1, device_id={"tp": lax.rem(x + o, tp_size), "dp": d, "rep": z}, device_id_type=MESH
        )

    @pl.when(z > 0)
    def _():
        pl.semaphore_signal(barrier, 1, device_id=z_device(-1), device_id_type=MESH)

    @pl.when(z < last)
    def _():
        pl.semaphore_signal(barrier, 1, device_id=z_device(1), device_id_type=MESH)

    load_down.wait()
    load_up.wait()
    tile = min(256, columns)

    def merge(k):
        layer, start = k % layers, k // layers * half
        load_weight(k).wait()

        def step(t, carry):
            at = pl.ds(pl.multiple_of(t * tile, tile), tile)
            low = lax.dot_general(
                dbuf[layer, :, pl.ds(start, half)], ubuf[layer, :, at], (((0,), (0,)), ((), ())),
                preferred_element_type=jnp.float32,
            )
            wide = wbuf[me, layer, pl.ds(start, half), at].astype(jnp.float32) + low
            wbuf[me, layer, pl.ds(start, half), at] = wide.astype(wbuf.dtype)
            return carry

        lax.fori_loop(0, columns // tile, step, 0)

    neighbours = jnp.where(z > 0, 1, 0) + jnp.where(z < last, 1, 0)

    def send_chunk(j, b, act):
        for o in range(1, tp_size):
            act(
                remote(
                    pbuf.at[b], psend.at[(o - 1) * dp_size * rep_size + b], parrive.at[b],
                    {"tp": lax.rem(x + o, tp_size), "dp": d, "rep": z},
                )
            )

    for k in range(count):
        merge(k)
        if k == 0:
            pl.semaphore_wait(barrier, neighbours + (1 + y_size - 1 + tp_size - 1))
        else:
            forward(0, z, jnp.int32(k - 1))
    for j, b in own_chunks[:1]:
        load_chunk(j, b).wait()
        send_chunk(j, b, lambda copy: copy.start())
    forward(0, z, jnp.int32(count - 1))
    for j, b in own_chunks[1:]:
        load_chunk(j, b).wait()
        send_chunk(j, b, lambda copy: copy.start())

    acc[...] = jnp.zeros_like(acc)
    squares[...] = jnp.zeros_like(squares)

    def wait_chunk(b):
        @pl.when(b // (groups * rep_size) != x)
        def _():
            remote(pbuf.at[b], psend.at[0], parrive.at[b], partner).wait_recv()

    def compute(b, k):
        layer = lax.rem(k, layers)
        at = pl.ds(pl.multiple_of(k // layers * half, half), half)
        weight = wbuf[b, layer, at, :]
        acc[layer] += jnp.dot(pbuf[b, :, at], weight, preferred_element_type=jnp.float32)
        wide = weight.astype(jnp.float32)
        squares[layer] += jnp.sum((wide * wide).reshape(half // 8, 8, columns), axis=0)

    def blocks_of(q, zz):
        return block(column(q // 2), lax.rem(c + q, 2), zz)

    def consume(zz, k, first, end, fresh):
        def step(q, carry):
            b = blocks_of(q, zz)
            if fresh is not None:
                @pl.when(fresh)
                def _():
                    wait_chunk(b)

            @pl.when(lax.rem(q, 2) == 1)
            def _():
                wait_piece(b, k)

            compute(b, k)
            return carry

        lax.fori_loop(first, end, step, 0)

    total = last * count

    def z_duty(j):
        zz, k = plane(1 + j // count), lax.rem(j, count)
        onz = doubled(zz, k)

        @pl.when(middle | jnp.logical_not(onz))
        def _():
            duty(0, zz, k)

        @pl.when(middle & onz)
        def _():
            for o in range(1, y_size):
                duty(o, zz, k)

    lead = jnp.where(middle, count, 0)

    def ahead(j, carry):
        z_duty(j)
        return carry

    lax.fori_loop(0, lead, ahead, 0)

    def substep(m, carry):
        i, k = m // count, lax.rem(m, count)

        @pl.when(m + lead < total)
        def _():
            z_duty(m + lead)

        zz = plane(i)

        @pl.when((i == 0) | jnp.logical_not(doubled(zz, k)))
        def _():
            for o in range(1, y_size):
                duty(o, zz, k)

        consume(zz, k, 0, 2 * y_size, k == 0)
        return carry

    lax.fori_loop(0, total, substep, 0)

    far = plane(last)
    for q in range(2 * y_size):
        wait_chunk(blocks_of(q, far))

    def early(k, carry):
        consume(far, k, 0, 2, None)
        return carry

    lax.fori_loop(0, layers, early, 0)
    band = min(128, tokens)

    def finish(layer, carry):
        def late(part, inner):
            o_first = jnp.where(part == 0, 0, 2)
            o_end = jnp.where(part == 0, 2, 2 * y_size)
            k = jnp.where(part == 2, layer, layers + layer)

            @pl.when((part == 0) & jnp.logical_not(middle))
            def _():
                duty(0, far, k)

            @pl.when((part == 2) | ((part == 1) & jnp.logical_not(middle)))
            def _():
                for o in range(1, y_size):
                    duty(o, far, k)

            consume(far, k, o_first, o_end, None)
            return inner

        lax.fori_loop(0, 3, late, 0)
        norm = jnp.sqrt(jnp.sum(squares[layer], axis=0, keepdims=True) + epsilon)
        factor = magnitude_ref[pl.ds(layer, 1), :] / norm

        def scale(t, inner):
            at = pl.ds(pl.multiple_of(t * band, band), band)
            out_ref[layer, at, :] = (acc[layer, at, :] * factor).astype(out_ref.dtype)
            return inner

        lax.fori_loop(0, tokens // band, scale, 0)
        return carry

    lax.fori_loop(0, layers, finish, 0)

    def drain(t, carry):
        for o in range(y_size):
            copies(o, t // count, lax.rem(t, count), lambda copy: copy.wait_send())
        return carry

    lax.fori_loop(0, rep_size * count, drain, 0)
    for j, b in own_chunks:
        send_chunk(j, b, lambda copy: copy.wait_send())


def local(sizes, prompts, frozen_projection_weight, lowrank_down_factor, lowrank_up_factor, magnitude):
    tp_size, dp_size, rep_size = sizes
    layers, rows, columns = frozen_projection_weight.shape
    rank = lowrank_down_factor.shape[2]
    tokens = prompts.shape[0]
    blocks = dp_size * rep_size
    y_size = dp_size // 2
    count = 2 * layers
    dma = pltpu.SemaphoreType.DMA
    return pl.pallas_call(
        functools.partial(kernel, sizes),
        out_shape=jax.ShapeDtypeStruct((layers, tokens, columns), jnp.bfloat16),
        in_specs=[pl.BlockSpec(memory_space=pl.ANY)] * 4 + [pl.BlockSpec(memory_space=pltpu.VMEM)],
        out_specs=pl.BlockSpec(memory_space=pltpu.VMEM),
        scratch_shapes=[
            pltpu.VMEM((blocks, layers, rows, columns), jnp.bfloat16),
            pltpu.VMEM((blocks, tokens, rows), jnp.bfloat16),
            pltpu.VMEM((layers, rank, rows), jnp.bfloat16),
            pltpu.VMEM((layers, rank, columns), jnp.bfloat16),
            pltpu.VMEM((layers, tokens, columns), jnp.float32),
            pltpu.VMEM((layers, 8, columns), jnp.float32),
            dma((blocks * count,)),
            dma((y_size * rep_size * count,)),
            dma((y_size * rep_size * count,)),
            dma((max(1, (y_size - 1) * rep_size * count),)),
            dma((y_size * rep_size * count,)),
            dma((max(1, (tp_size - 1) * blocks),)),
            dma((blocks,)),
            dma((blocks,)),
            dma((count,)),
            dma((2,)),
        ],
        compiler_params=pltpu.CompilerParams(
            collective_id=0, has_side_effects=True, vmem_limit_bytes=66_000_000
        ),
        cost_estimate=pl.CostEstimate(
            flops=2 * layers * tokens * columns * rows * blocks, bytes_accessed=2 * blocks * rows * columns,
            transcendentals=0,
        ),
    )(prompts, frozen_projection_weight, jnp.swapaxes(lowrank_down_factor, 1, 2), lowrank_up_factor, magnitude)


def solution(mesh):
    in_specs = (
        P(("dp", "rep"), "tp"),
        P(None, ("dp", "rep"), "tp"),
        P(None, ("dp", "rep"), None),
        P(None, None, "tp"),
        P(None, "tp"),
    )
    out_specs = P(None, ("dp", "rep"), "tp")
    sizes = tuple(mesh.shape[name] for name in ("tp", "dp", "rep"))
    return jax.shard_map(
        functools.partial(local, sizes), mesh=mesh, in_specs=in_specs, out_specs=out_specs, check_vma=False
    )
```

```python
import functools

import jax
import jax.numpy as jnp
from jax import lax
from jax.experimental import pallas as pl
from jax.experimental.pallas import tpu as pltpu
from jax.sharding import PartitionSpec as P

epsilon = 1e-06
MESH = pl.DeviceIdType.MESH


def kernel(
    sizes, prompts_ref, weight_ref, down_ref, up_ref, magnitude_ref, out_ref,
    wbuf, pbuf, dbuf, ubuf, acc, squares,
    arrive, zup, zdown, ysend, csend, psend, parrive, load_p, load_w, load_f,
):
    tp_size, dp_size, rep_size = sizes
    y_size = dp_size // 2
    layers, rows, columns = weight_ref.shape
    tokens = prompts_ref.shape[0]
    half = rows // 2
    width = columns // 2
    count = 2 * layers
    groups = dp_size // tp_size
    x = lax.axis_index("tp")
    d = lax.axis_index("dp")
    z = lax.axis_index("rep")
    y, c = d // 2, lax.rem(d, 2)
    partner = {"tp": x, "dp": d + 1 - 2 * c, "rep": z}
    last = rep_size - 1
    middle = (z > 0) & (z < last)

    def column(o):
        return lax.rem(y + o, y_size)

    def block(yy, cc, zz):
        return (yy * 2 + cc) * rep_size + zz

    def piece(b, k, h):
        start = pl.multiple_of(k // layers * half, half)
        return wbuf.at[b, lax.rem(k, layers), pl.ds(start, half), pl.ds(h * width, width)]

    def ranked(at):
        longer = -1 if at > last - at else 1
        return sorted(range(rep_size), key=lambda k: (abs(k - at), -longer * (k - at)))

    table = [ranked(at) for at in range(rep_size)]

    def plane(i):
        value = jnp.int32(0)
        for at in range(rep_size):
            for step in range(rep_size):
                value = jnp.where((z == at) & (i == step), jnp.int32(table[at][step]), value)
        return value

    def doubled(zz, k):
        return ((zz == 0) | (zz == last)) & (k >= layers)

    def y_device(o):
        return {"tp": x, "dp": column(o) * 2 + c, "rep": z}

    def z_device(step):
        return {"tp": x, "dp": d, "rep": z + step}

    def remote(ref, send_sem, recv_sem, device):
        return pltpu.make_async_remote_copy(
            src_ref=ref, dst_ref=ref, send_sem=send_sem, recv_sem=recv_sem,
            device_id=device, device_id_type=MESH,
        )

    def wait_piece(b, k, h):
        remote(piece(b, k, h), csend.at[0], arrive.at[(b * count + k) * 2 + h], partner).wait_recv()

    def copies(o, zz, k, h, act):
        yy = column(o)
        b = block(yy, c, zz)
        ref, landed = piece(b, k, h), arrive.at[(b * count + k) * 2 + h]
        at = ((yy * rep_size + zz) * count + k) * 2 + h
        onz = doubled(zz, k)
        along = onz if o > 0 else (z >= 0)

        @pl.when(along & (zz >= z) & (z > 0))
        def _():
            act(remote(ref, zdown.at[at], landed, z_device(-1)))

        @pl.when(along & (zz <= z) & (z < last))
        def _():
            act(remote(ref, zup.at[at], landed, z_device(1)))

        if o == 0:
            for p in range(1, y_size):
                @pl.when((zz == z) | jnp.logical_not(onz))
                def _(p=p):
                    act(remote(ref, ysend.at[(((p - 1) * rep_size + zz) * count + k) * 2 + h], landed, y_device(p)))

        act(remote(ref, csend.at[at], landed, partner))

    def forward(o, zz, k, h):
        copies(o, zz, k, h, lambda copy: copy.start())

    def duty(o, zz, k, halves=(0, 1)):
        for h in halves:
            wait_piece(block(column(o), c, zz), k, h)
            forward(o, zz, k, h)

    me = block(y, c, z)

    def load_weight(k):
        at = pl.ds(k // layers * half, half)
        return pltpu.make_async_copy(
            weight_ref.at[k % layers, at, :], wbuf.at[me, k % layers, at, :], load_w.at[k]
        )

    load_down = pltpu.make_async_copy(down_ref, dbuf, load_f.at[0])
    load_up = pltpu.make_async_copy(up_ref, ubuf, load_f.at[1])
    load_down.start()
    load_up.start()
    for k in range(count):
        load_weight(k).start()

    own_chunks = []
    for i in range(rep_size):
        for g in range(groups):
            zz = plane(i)
            own_chunks.append((g * rep_size + zz, x * groups * rep_size + g * rep_size + zz))

    def load_chunk(j, b):
        start = pl.multiple_of(j * rows, rows)
        return pltpu.make_async_copy(prompts_ref.at[:, pl.ds(start, rows)], pbuf.at[b], load_p.at[b])

    for j, b in own_chunks:
        load_chunk(j, b).start()

    barrier = pltpu.get_barrier_semaphore()
    pl.semaphore_signal(barrier, 1, device_id=partner, device_id_type=MESH)
    for o in range(1, y_size):
        pl.semaphore_signal(barrier, 1, device_id=y_device(o), device_id_type=MESH)
    for o in range(1, tp_size):
        pl.semaphore_signal(
            barrier, 1, device_id={"tp": lax.rem(x + o, tp_size), "dp": d, "rep": z}, device_id_type=MESH
        )

    @pl.when(z > 0)
    def _():
        pl.semaphore_signal(barrier, 1, device_id=z_device(-1), device_id_type=MESH)

    @pl.when(z < last)
    def _():
        pl.semaphore_signal(barrier, 1, device_id=z_device(1), device_id_type=MESH)

    load_down.wait()
    load_up.wait()
    tile = min(512, columns)

    def merge(k):
        layer, start = k % layers, k // layers * half
        load_weight(k).wait()

        def step(t, carry):
            at = pl.ds(pl.multiple_of(t * tile, tile), tile)
            low = lax.dot_general(
                dbuf[layer, :, pl.ds(start, half)], ubuf[layer, :, at], (((0,), (0,)), ((), ())),
                preferred_element_type=jnp.float32,
            )
            wide = wbuf[me, layer, pl.ds(start, half), at].astype(jnp.float32) + low
            wbuf[me, layer, pl.ds(start, half), at] = wide.astype(wbuf.dtype)
            return carry

        lax.fori_loop(0, columns // tile, step, 0)

    neighbours = jnp.where(z > 0, 1, 0) + jnp.where(z < last, 1, 0)

    def send_chunk(n, act):
        j, b = own_chunks[n]
        for o in range(1, tp_size):
            act(
                remote(
                    pbuf.at[b], psend.at[(o - 1) * len(own_chunks) + n], parrive.at[b],
                    {"tp": lax.rem(x + o, tp_size), "dp": d, "rep": z},
                )
            )

    def start_chunk(n):
        load_chunk(*own_chunks[n]).wait()
        send_chunk(n, lambda copy: copy.start())

    for k in range(count):
        merge(k)
        if k == 0:
            pl.semaphore_wait(barrier, neighbours + (1 + y_size - 1 + tp_size - 1))
        else:
            for h in range(2):
                forward(0, z, jnp.int32(k - 1), h)
    start_chunk(0)
    for h in range(2):
        forward(0, z, jnp.int32(count - 1), h)
    for n in range(1, len(own_chunks)):
        start_chunk(n)

    acc[...] = jnp.zeros_like(acc)
    squares[...] = jnp.zeros_like(squares)

    def wait_chunk(b):
        @pl.when(b // (groups * rep_size) != x)
        def _():
            remote(pbuf.at[b], psend.at[0], parrive.at[b], partner).wait_recv()

    def compute(b, layer, at, cols):
        weight = wbuf[b, layer, at, cols]
        acc[layer, :, cols] += jnp.dot(pbuf[b, :, at], weight, preferred_element_type=jnp.float32)
        wide = weight.astype(jnp.float32)
        squares[layer, :, cols] += jnp.sum((wide * wide).reshape(-1, 8, wide.shape[1]), axis=0)

    def blocks_of(q, zz):
        return block(column(q // 2), lax.rem(c + q, 2), zz)

    def consume(zz, k, fresh):
        at = pl.ds(pl.multiple_of(k // layers * half, half), half)

        def step(q, carry):
            b = blocks_of(q, zz)

            @pl.when(fresh)
            def _():
                wait_chunk(b)

            @pl.when(lax.rem(q, 2) == 1)
            def _():
                for h in range(2):
                    wait_piece(b, k, h)

            compute(b, lax.rem(k, layers), at, slice(None))
            return carry

        lax.fori_loop(0, 2 * y_size, step, 0)

    total = last * count

    def z_duty(j):
        zz, k = plane(1 + j // count), lax.rem(j, count)
        onz = doubled(zz, k)

        @pl.when(middle | jnp.logical_not(onz))
        def _():
            duty(0, zz, k)

        @pl.when(middle & onz)
        def _():
            for o in range(1, y_size):
                duty(o, zz, k)

    lead = jnp.where(middle, count, 0)

    def ahead(j, carry):
        z_duty(j)
        return carry

    lax.fori_loop(0, lead, ahead, 0)

    def substep(m, carry):
        i, k = m // count, lax.rem(m, count)

        @pl.when(m + lead < total)
        def _():
            z_duty(m + lead)

        zz = plane(i)

        @pl.when((i == 0) | jnp.logical_not(doubled(zz, k)))
        def _():
            for o in range(1, y_size):
                duty(o, zz, k)

        consume(zz, k, k == 0)
        return carry

    lax.fori_loop(0, total, substep, 0)

    far = plane(last)
    for q in range(2 * y_size):
        wait_chunk(blocks_of(q, far))

    def drain(zz, k):
        for o in range(y_size):
            for h in range(2):
                copies(o, zz, k, h, lambda copy: copy.wait_send())

    def drain_plane(t, carry):
        drain(plane(t // count), lax.rem(t, count))
        return carry

    lax.fori_loop(0, total, drain_plane, 0)
    for n in range(len(own_chunks)):
        send_chunk(n, lambda copy: copy.wait_send())
    band = min(128, tokens)

    def gather(layer, first, end, halves):
        cols = pl.ds(halves[0] * width, len(halves) * width)

        def step(q, carry):
            b = blocks_of(q, far)

            @pl.when(lax.rem(q, 2) == 1)
            def _():
                for h in halves:
                    wait_piece(b, layer, h)
                    wait_piece(b, layers + layer, h)

            compute(b, layer, slice(None), cols)
            return carry

        lax.fori_loop(first, end, step, 0)

    def finish(layer, carry):
        @pl.when(jnp.logical_not(middle))
        def _():
            duty(0, far, layers + layer)

        gather(layer, 0, 2, (0, 1))

        @pl.when(layer > 0)
        def _():
            drain(far, layer - 1)
            drain(far, layers + layer - 1)

        for h in range(2):
            for o in range(1, y_size):
                duty(o, far, layer, (h,))

                @pl.when(jnp.logical_not(middle))
                def _(o=o):
                    duty(o, far, layers + layer, (h,))

            gather(layer, 2, 2 * y_size, (h,))
            cols = pl.ds(h * width, width)
            norm = jnp.sqrt(jnp.sum(squares[layer, :, cols], axis=0, keepdims=True) + epsilon)
            factor = magnitude_ref[pl.ds(layer, 1), :][:, h * width:(h + 1) * width] / norm

            def scale(t, inner, cols=cols, factor=factor):
                at = pl.ds(pl.multiple_of(t * band, band), band)
                out_ref[layer, at, cols] = (acc[layer, at, cols] * factor).astype(out_ref.dtype)
                return inner

            lax.fori_loop(0, tokens // band, scale, 0)
        return carry

    lax.fori_loop(0, layers, finish, 0)
    drain(far, layers - 1)
    drain(far, count - 1)


def local(sizes, prompts, frozen_projection_weight, lowrank_down_factor, lowrank_up_factor, magnitude):
    tp_size, dp_size, rep_size = sizes
    layers, rows, columns = frozen_projection_weight.shape
    rank = lowrank_down_factor.shape[2]
    tokens = prompts.shape[0]
    blocks = dp_size * rep_size
    y_size = dp_size // 2
    count = 2 * layers
    dma = pltpu.SemaphoreType.DMA
    return pl.pallas_call(
        functools.partial(kernel, sizes),
        out_shape=pltpu.VMEM((layers, tokens, columns), jnp.bfloat16),
        in_specs=[pl.BlockSpec(memory_space=pl.ANY)] * 4 + [pl.BlockSpec(memory_space=pltpu.VMEM)],
        out_specs=pl.BlockSpec(memory_space=pltpu.VMEM),
        scratch_shapes=[
            pltpu.VMEM((blocks, layers, rows, columns), jnp.bfloat16),
            pltpu.VMEM((blocks, tokens, rows), jnp.bfloat16),
            pltpu.VMEM((layers, rank, rows), jnp.bfloat16),
            pltpu.VMEM((layers, rank, columns), jnp.bfloat16),
            pltpu.VMEM((layers, tokens, columns), jnp.float32),
            pltpu.VMEM((layers, 8, columns), jnp.float32),
            dma((blocks * count * 2,)),
            dma((y_size * rep_size * count * 2,)),
            dma((y_size * rep_size * count * 2,)),
            dma((max(1, (y_size - 1) * rep_size * count * 2),)),
            dma((y_size * rep_size * count * 2,)),
            dma((max(1, (tp_size - 1) * (blocks // tp_size)),)),
            dma((blocks,)),
            dma((blocks,)),
            dma((count,)),
            dma((2,)),
        ],
        compiler_params=pltpu.CompilerParams(
            collective_id=0, has_side_effects=True, vmem_limit_bytes=58_000_000
        ),
        cost_estimate=pl.CostEstimate(
            flops=2 * layers * tokens * columns * rows * blocks, bytes_accessed=2 * blocks * rows * columns,
            transcendentals=0,
        ),
    )(prompts, frozen_projection_weight, jnp.swapaxes(lowrank_down_factor, 1, 2), lowrank_up_factor, magnitude)


def solution(mesh):
    in_specs = (
        P(("dp", "rep"), "tp"),
        P(None, ("dp", "rep"), "tp"),
        P(None, ("dp", "rep"), None),
        P(None, None, "tp"),
        P(None, "tp"),
    )
    out_specs = P(None, ("dp", "rep"), "tp")
    sizes = tuple(mesh.shape[name] for name in ("tp", "dp", "rep"))
    return jax.shard_map(
        functools.partial(local, sizes), mesh=mesh, in_specs=in_specs, out_specs=out_specs, check_vma=False
    )
```

```python
import functools

import jax
import jax.numpy as jnp
from jax import lax
from jax.experimental import pallas as pl
from jax.experimental.pallas import tpu as pltpu
from jax.sharding import PartitionSpec as P

epsilon = 1e-06
MESH = pl.DeviceIdType.MESH


def kernel(
    sizes, prompts_ref, weight_ref, down_ref, up_ref, magnitude_ref, out_ref,
    wbuf, pbuf, dbuf, ubuf, mbuf, acc, squares,
    arrive, zup, zdown, ysend, csend, psend, parrive, load_p, load_w, load_f,
):
    tp_size, dp_size, rep_size = sizes
    y_size = dp_size // 2
    layers, rows, columns = weight_ref.shape
    tokens = prompts_ref.shape[0]
    half = rows // 2
    width = columns // 2
    count = 2 * layers
    groups = dp_size // tp_size
    x = lax.axis_index("tp")
    d = lax.axis_index("dp")
    z = lax.axis_index("rep")
    y, c = d // 2, lax.rem(d, 2)
    partner = {"tp": x, "dp": d + 1 - 2 * c, "rep": z}
    last = rep_size - 1
    middle = (z > 0) & (z < last)

    def column(o):
        return lax.rem(y + o, y_size)

    def block(yy, cc, zz):
        return (yy * 2 + cc) * rep_size + zz

    def piece(b, k, h):
        start = pl.multiple_of(k // layers * half, half)
        return wbuf.at[b, lax.rem(k, layers), pl.ds(start, half), pl.ds(h * width, width)]

    def ranked(at):
        longer = -1 if at > last - at else 1
        return sorted(range(rep_size), key=lambda k: (abs(k - at), -longer * (k - at)))

    table = [ranked(at) for at in range(rep_size)]

    def plane(i):
        value = jnp.int32(0)
        for at in range(rep_size):
            for step in range(rep_size):
                value = jnp.where((z == at) & (i == step), jnp.int32(table[at][step]), value)
        return value

    def doubled(zz, k):
        return ((zz == 0) | (zz == last)) & (k >= layers)

    def y_device(o):
        return {"tp": x, "dp": column(o) * 2 + c, "rep": z}

    def z_device(step):
        return {"tp": x, "dp": d, "rep": z + step}

    def remote(ref, send_sem, recv_sem, device):
        return pltpu.make_async_remote_copy(
            src_ref=ref, dst_ref=ref, send_sem=send_sem, recv_sem=recv_sem,
            device_id=device, device_id_type=MESH,
        )

    def wait_piece(b, k, h):
        remote(piece(b, k, h), csend.at[0], arrive.at[(b * count + k) * 2 + h], partner).wait_recv()

    def copies(o, zz, k, h, act):
        yy = column(o)
        b = block(yy, c, zz)
        ref, landed = piece(b, k, h), arrive.at[(b * count + k) * 2 + h]
        at = ((yy * rep_size + zz) * count + k) * 2 + h
        onz = doubled(zz, k)
        along = onz if o > 0 else (z >= 0)

        @pl.when(along & (zz >= z) & (z > 0))
        def _():
            act(remote(ref, zdown.at[at], landed, z_device(-1)))

        @pl.when(along & (zz <= z) & (z < last))
        def _():
            act(remote(ref, zup.at[at], landed, z_device(1)))

        if o == 0:
            for p in range(1, y_size):
                @pl.when((zz == z) | jnp.logical_not(onz))
                def _(p=p):
                    act(remote(ref, ysend.at[(((p - 1) * rep_size + zz) * count + k) * 2 + h], landed, y_device(p)))

        act(remote(ref, csend.at[at], landed, partner))

    def forward(o, zz, k, h):
        copies(o, zz, k, h, lambda copy: copy.start())

    def duty(o, zz, k, halves=(0, 1)):
        for h in halves:
            wait_piece(block(column(o), c, zz), k, h)
            forward(o, zz, k, h)

    me = block(y, c, z)

    def load_weight(k):
        at = pl.ds(k // layers * half, half)
        return pltpu.make_async_copy(
            weight_ref.at[k % layers, at, :], wbuf.at[me, k % layers, at, :], load_w.at[k]
        )

    load_down = pltpu.make_async_copy(down_ref, dbuf, load_f.at[0])
    load_up = pltpu.make_async_copy(up_ref, ubuf, load_f.at[1])
    load_magnitude = pltpu.make_async_copy(magnitude_ref, mbuf, load_f.at[2])
    load_weight(0).start()
    load_down.start()
    load_up.start()
    for k in range(1, count):
        load_weight(k).start()
    load_magnitude.start()

    barrier = pltpu.get_barrier_semaphore()
    pl.semaphore_signal(barrier, 1, device_id=partner, device_id_type=MESH)
    for o in range(1, y_size):
        pl.semaphore_signal(barrier, 1, device_id=y_device(o), device_id_type=MESH)
    for o in range(1, tp_size):
        pl.semaphore_signal(
            barrier, 1, device_id={"tp": lax.rem(x + o, tp_size), "dp": d, "rep": z}, device_id_type=MESH
        )

    @pl.when(z > 0)
    def _():
        pl.semaphore_signal(barrier, 1, device_id=z_device(-1), device_id_type=MESH)

    @pl.when(z < last)
    def _():
        pl.semaphore_signal(barrier, 1, device_id=z_device(1), device_id_type=MESH)

    own_chunks = []
    for i in range(rep_size):
        for g in range(groups):
            zz = plane(i)
            own_chunks.append((g * rep_size + zz, x * groups * rep_size + g * rep_size + zz))

    def load_chunk(j, b):
        start = pl.multiple_of(j * rows, rows)
        return pltpu.make_async_copy(prompts_ref.at[:, pl.ds(start, rows)], pbuf.at[b], load_p.at[b])

    load_down.wait()
    load_up.wait()
    tile = min(512, columns)

    def merge(k):
        layer, start = k % layers, k // layers * half
        load_weight(k).wait()

        def step(t, carry):
            at = pl.ds(pl.multiple_of(t * tile, tile), tile)
            low = lax.dot_general(
                dbuf[layer, :, pl.ds(start, half)], ubuf[layer, :, at], (((0,), (0,)), ((), ())),
                preferred_element_type=jnp.float32,
            )
            wide = wbuf[me, layer, pl.ds(start, half), at].astype(jnp.float32) + low
            wbuf[me, layer, pl.ds(start, half), at] = wide.astype(wbuf.dtype)
            return carry

        lax.fori_loop(0, columns // tile, step, 0)

    neighbours = jnp.where(z > 0, 1, 0) + jnp.where(z < last, 1, 0)

    def send_chunk(n, act):
        j, b = own_chunks[n]
        for o in range(1, tp_size):
            act(
                remote(
                    pbuf.at[b], psend.at[(o - 1) * len(own_chunks) + n], parrive.at[b],
                    {"tp": lax.rem(x + o, tp_size), "dp": d, "rep": z},
                )
            )

    def start_chunk(n):
        load_chunk(*own_chunks[n]).wait()
        send_chunk(n, lambda copy: copy.start())

    for k in range(count):
        merge(k)
        if k == 0:
            for j, b in own_chunks:
                load_chunk(j, b).start()
            pl.semaphore_wait(barrier, neighbours + (1 + y_size - 1 + tp_size - 1))
        else:
            for h in range(2):
                forward(0, z, jnp.int32(k - 1), h)
    start_chunk(0)
    for h in range(2):
        forward(0, z, jnp.int32(count - 1), h)
    for n in range(1, len(own_chunks)):
        start_chunk(n)

    acc[...] = jnp.zeros_like(acc)
    squares[...] = jnp.zeros_like(squares)

    def wait_chunk(b):
        @pl.when(b // (groups * rep_size) != x)
        def _():
            remote(pbuf.at[b], psend.at[0], parrive.at[b], partner).wait_recv()

    def compute(b, layer, at, cols):
        weight = wbuf[b, layer, at, cols]
        acc[layer, :, cols] += jnp.dot(pbuf[b, :, at], weight, preferred_element_type=jnp.float32)
        wide = weight.astype(jnp.float32)
        squares[layer, :, cols] += jnp.sum((wide * wide).reshape(-1, 8, wide.shape[1]), axis=0)

    def blocks_of(q, zz):
        return block(column(q // 2), lax.rem(c + q, 2), zz)

    def consume(zz, k, fresh):
        at = pl.ds(pl.multiple_of(k // layers * half, half), half)

        def step(q, carry):
            b = blocks_of(q, zz)

            @pl.when(fresh)
            def _():
                wait_chunk(b)

            @pl.when(lax.rem(q, 2) == 1)
            def _():
                for h in range(2):
                    wait_piece(b, k, h)

            compute(b, lax.rem(k, layers), at, slice(None))
            return carry

        lax.fori_loop(0, 2 * y_size, step, 0)

    total = last * count

    def z_duty(j):
        zz, k = plane(1 + j // count), lax.rem(j, count)
        onz = doubled(zz, k)

        @pl.when(middle | jnp.logical_not(onz))
        def _():
            duty(0, zz, k)

        @pl.when(middle & onz)
        def _():
            for o in range(1, y_size):
                duty(o, zz, k)

    lead = jnp.where(middle, count, 0)

    def ahead(j, carry):
        z_duty(j)
        return carry

    lax.fori_loop(0, lead, ahead, 0)

    def substep(m, carry):
        i, k = m // count, lax.rem(m, count)

        @pl.when(m + lead < total)
        def _():
            z_duty(m + lead)

        zz = plane(i)

        @pl.when((i == 0) | jnp.logical_not(doubled(zz, k)))
        def _():
            for o in range(1, y_size):
                duty(o, zz, k)

        consume(zz, k, k == 0)
        return carry

    lax.fori_loop(0, total, substep, 0)

    load_magnitude.wait()
    far = plane(last)
    for q in range(2 * y_size):
        wait_chunk(blocks_of(q, far))

    def drain(zz, k):
        for o in range(y_size):
            for h in range(2):
                copies(o, zz, k, h, lambda copy: copy.wait_send())

    def drain_plane(t, carry):
        drain(plane(t // count), lax.rem(t, count))
        return carry

    lax.fori_loop(0, total, drain_plane, 0)
    for n in range(len(own_chunks)):
        send_chunk(n, lambda copy: copy.wait_send())
    band = min(128, tokens)

    def gather(layer, first, end, halves):
        cols = pl.ds(halves[0] * width, len(halves) * width)

        def step(q, carry):
            b = blocks_of(q, far)

            @pl.when(lax.rem(q, 2) == 1)
            def _():
                for h in halves:
                    wait_piece(b, layer, h)
                    wait_piece(b, layers + layer, h)

            compute(b, layer, slice(None), cols)
            return carry

        lax.fori_loop(first, end, step, 0)

    def finish(layer, carry):
        @pl.when(jnp.logical_not(middle))
        def _():
            duty(0, far, layers + layer)

        gather(layer, 0, 2, (0, 1))

        @pl.when(layer > 0)
        def _():
            drain(far, layer - 1)
            drain(far, layers + layer - 1)

        for h in range(2):
            for o in range(1, y_size):
                duty(o, far, layer, (h,))

                @pl.when(jnp.logical_not(middle))
                def _(o=o):
                    duty(o, far, layers + layer, (h,))

            gather(layer, 2, 2 * y_size, (h,))
            cols = pl.ds(h * width, width)
            norm = jnp.sqrt(jnp.sum(squares[layer, :, cols], axis=0, keepdims=True) + epsilon)
            factor = mbuf[pl.ds(layer, 1), :][:, h * width:(h + 1) * width] / norm

            def scale(t, inner, cols=cols, factor=factor):
                at = pl.ds(pl.multiple_of(t * band, band), band)
                out_ref[layer, at, cols] = (acc[layer, at, cols] * factor).astype(out_ref.dtype)
                return inner

            lax.fori_loop(0, tokens // band, scale, 0)
        return carry

    lax.fori_loop(0, layers, finish, 0)
    drain(far, layers - 1)
    drain(far, count - 1)


def local(sizes, prompts, frozen_projection_weight, lowrank_down_factor, lowrank_up_factor, magnitude):
    tp_size, dp_size, rep_size = sizes
    layers, rows, columns = frozen_projection_weight.shape
    rank = lowrank_down_factor.shape[2]
    tokens = prompts.shape[0]
    blocks = dp_size * rep_size
    y_size = dp_size // 2
    count = 2 * layers
    dma = pltpu.SemaphoreType.DMA
    return pl.pallas_call(
        functools.partial(kernel, sizes),
        out_shape=pltpu.VMEM((layers, tokens, columns), jnp.bfloat16),
        in_specs=[pl.BlockSpec(memory_space=pl.ANY)] * 5,
        out_specs=pl.BlockSpec(memory_space=pltpu.VMEM),
        scratch_shapes=[
            pltpu.VMEM((blocks, layers, rows, columns), jnp.bfloat16),
            pltpu.VMEM((blocks, tokens, rows), jnp.bfloat16),
            pltpu.VMEM((layers, rank, rows), jnp.bfloat16),
            pltpu.VMEM((layers, rank, columns), jnp.bfloat16),
            pltpu.VMEM((layers, columns), jnp.float32),
            pltpu.VMEM((layers, tokens, columns), jnp.float32),
            pltpu.VMEM((layers, 8, columns), jnp.float32),
            dma((blocks * count * 2,)),
            dma((y_size * rep_size * count * 2,)),
            dma((y_size * rep_size * count * 2,)),
            dma((max(1, (y_size - 1) * rep_size * count * 2),)),
            dma((y_size * rep_size * count * 2,)),
            dma((max(1, (tp_size - 1) * (blocks // tp_size)),)),
            dma((blocks,)),
            dma((blocks,)),
            dma((count,)),
            dma((3,)),
        ],
        compiler_params=pltpu.CompilerParams(
            collective_id=0, has_side_effects=True, vmem_limit_bytes=61_000_000
        ),
        cost_estimate=pl.CostEstimate(
            flops=2 * layers * tokens * columns * rows * blocks, bytes_accessed=2 * blocks * rows * columns,
            transcendentals=0,
        ),
    )(prompts, frozen_projection_weight, jnp.swapaxes(lowrank_down_factor, 1, 2), lowrank_up_factor, magnitude)


def solution(mesh):
    in_specs = (
        P(("dp", "rep"), "tp"),
        P(None, ("dp", "rep"), "tp"),
        P(None, ("dp", "rep"), None),
        P(None, None, "tp"),
        P(None, "tp"),
    )
    out_specs = P(None, ("dp", "rep"), "tp")
    sizes = tuple(mesh.shape[name] for name in ("tp", "dp", "rep"))
    return jax.shard_map(
        functools.partial(local, sizes), mesh=mesh, in_specs=in_specs, out_specs=out_specs, check_vma=False
    )
```

```python
import functools

import jax
import jax.numpy as jnp
from jax import lax
from jax.experimental import pallas as pl
from jax.experimental.pallas import tpu as pltpu
from jax.sharding import PartitionSpec as P

epsilon = 1e-06
MESH = pl.DeviceIdType.MESH


def kernel(
    sizes, prompts_ref, weight_ref, down_ref, up_ref, magnitude_ref, out_ref,
    wbuf, pbuf, dbuf, ubuf, mbuf, acc, squares,
    arrive, zup, zdown, ysend, csend, psend, parrive, load_p, load_w, load_f,
):
    tp_size, dp_size, rep_size = sizes
    y_size = dp_size // 2
    layers, rows, columns = weight_ref.shape
    tokens = prompts_ref.shape[0]
    half = rows // 2
    width = columns // 2
    count = 2 * layers
    groups = dp_size // tp_size
    x = lax.axis_index("tp")
    d = lax.axis_index("dp")
    z = lax.axis_index("rep")
    y, c = d // 2, lax.rem(d, 2)
    partner = {"tp": x, "dp": d + 1 - 2 * c, "rep": z}
    last = rep_size - 1
    middle = (z > 0) & (z < last)

    def column(o):
        return lax.rem(y + o, y_size)

    def block(yy, cc, zz):
        return (yy * 2 + cc) * rep_size + zz

    def piece(b, k, h):
        start = pl.multiple_of(k // layers * half, half)
        return wbuf.at[b, lax.rem(k, layers), pl.ds(start, half), pl.ds(h * width, width)]

    def ranked(at):
        longer = -1 if at > last - at else 1
        return sorted(range(rep_size), key=lambda k: (abs(k - at), -longer * (k - at)))

    table = [ranked(at) for at in range(rep_size)]

    def plane(i):
        value = jnp.int32(0)
        for at in range(rep_size):
            for step in range(rep_size):
                value = jnp.where((z == at) & (i == step), jnp.int32(table[at][step]), value)
        return value

    def doubled(zz, k):
        return ((zz == 0) | (zz == last)) & (k >= layers)

    def y_device(o):
        return {"tp": x, "dp": column(o) * 2 + c, "rep": z}

    def z_device(step):
        return {"tp": x, "dp": d, "rep": z + step}

    def remote(ref, send_sem, recv_sem, device):
        return pltpu.make_async_remote_copy(
            src_ref=ref, dst_ref=ref, send_sem=send_sem, recv_sem=recv_sem,
            device_id=device, device_id_type=MESH,
        )

    def wait_piece(b, k, h):
        remote(piece(b, k, h), csend, arrive.at[(b * count + k) * 2 + h], partner).wait_recv()

    def forward(o, zz, k, h):
        yy = column(o)
        b = block(yy, c, zz)
        ref, landed = piece(b, k, h), arrive.at[(b * count + k) * 2 + h]
        onz = doubled(zz, k)
        along = onz if o > 0 else (z >= 0)

        @pl.when(along & (zz >= z) & (z > 0))
        def _():
            remote(ref, zdown, landed, z_device(-1)).start()

        @pl.when(along & (zz <= z) & (z < last))
        def _():
            remote(ref, zup, landed, z_device(1)).start()

        if o == 0:
            for p in range(1, y_size):
                @pl.when((zz == z) | jnp.logical_not(onz))
                def _(p=p):
                    remote(ref, ysend.at[p - 1], landed, y_device(p)).start()

        remote(ref, csend, landed, partner).start()

    def duty(o, zz, k, halves=(0, 1)):
        for h in halves:
            wait_piece(block(column(o), c, zz), k, h)
            forward(o, zz, k, h)

    me = block(y, c, z)

    def load_weight(k):
        at = pl.ds(k // layers * half, half)
        return pltpu.make_async_copy(
            weight_ref.at[k % layers, at, :], wbuf.at[me, k % layers, at, :], load_w.at[k]
        )

    load_down = pltpu.make_async_copy(down_ref, dbuf, load_f.at[0])
    load_up = pltpu.make_async_copy(up_ref, ubuf, load_f.at[1])
    load_magnitude = pltpu.make_async_copy(magnitude_ref, mbuf, load_f.at[2])
    load_weight(0).start()
    load_down.start()
    load_up.start()
    for k in range(1, count):
        load_weight(k).start()
    load_magnitude.start()

    barrier = pltpu.get_barrier_semaphore()
    pl.semaphore_signal(barrier, 1, device_id=partner, device_id_type=MESH)
    for o in range(1, y_size):
        pl.semaphore_signal(barrier, 1, device_id=y_device(o), device_id_type=MESH)
    for o in range(1, tp_size):
        pl.semaphore_signal(
            barrier, 1, device_id={"tp": lax.rem(x + o, tp_size), "dp": d, "rep": z}, device_id_type=MESH
        )

    @pl.when(z > 0)
    def _():
        pl.semaphore_signal(barrier, 1, device_id=z_device(-1), device_id_type=MESH)

    @pl.when(z < last)
    def _():
        pl.semaphore_signal(barrier, 1, device_id=z_device(1), device_id_type=MESH)

    own_chunks = []
    for i in range(rep_size):
        for g in range(groups):
            zz = plane(i)
            own_chunks.append((g * rep_size + zz, x * groups * rep_size + g * rep_size + zz))

    def load_chunk(n):
        j, b = own_chunks[n]
        start = pl.multiple_of(j * rows, rows)
        return pltpu.make_async_copy(prompts_ref.at[:, pl.ds(start, rows)], pbuf.at[b], load_p.at[n])

    load_down.wait()
    load_up.wait()
    tile = min(512, columns)

    def merge(k):
        layer, start = k % layers, k // layers * half
        load_weight(k).wait()

        def step(t, carry):
            at = pl.ds(pl.multiple_of(t * tile, tile), tile)
            low = lax.dot_general(
                dbuf[layer, :, pl.ds(start, half)], ubuf[layer, :, at], (((0,), (0,)), ((), ())),
                preferred_element_type=jnp.float32,
            )
            wide = wbuf[me, layer, pl.ds(start, half), at].astype(jnp.float32) + low
            wbuf[me, layer, pl.ds(start, half), at] = wide.astype(wbuf.dtype)
            return carry

        lax.fori_loop(0, columns // tile, step, 0)

    neighbours = jnp.where(z > 0, 1, 0) + jnp.where(z < last, 1, 0)

    def start_chunk(n):
        load_chunk(n).wait()
        b = own_chunks[n][1]
        for o in range(1, tp_size):
            remote(
                pbuf.at[b], psend.at[o - 1], parrive.at[b],
                {"tp": lax.rem(x + o, tp_size), "dp": d, "rep": z},
            ).start()

    for k in range(count):
        merge(k)
        if k == 0:
            for n in range(len(own_chunks)):
                load_chunk(n).start()
            pl.semaphore_wait(barrier, neighbours + (1 + y_size - 1 + tp_size - 1))
        else:
            for h in range(2):
                forward(0, z, jnp.int32(k - 1), h)
    start_chunk(0)
    for h in range(2):
        forward(0, z, jnp.int32(count - 1), h)
    for n in range(1, len(own_chunks)):
        start_chunk(n)

    acc[...] = jnp.zeros_like(acc)
    squares[...] = jnp.zeros_like(squares)

    def wait_chunk(b):
        @pl.when(b // (groups * rep_size) != x)
        def _():
            remote(pbuf.at[b], psend.at[0], parrive.at[b], partner).wait_recv()

    def compute(b, layer, at, cols):
        weight = wbuf[b, layer, at, cols]
        acc[layer, :, cols] += jnp.dot(pbuf[b, :, at], weight, preferred_element_type=jnp.float32)
        wide = weight.astype(jnp.float32)
        squares[layer, :, cols] += jnp.sum((wide * wide).reshape(-1, 8, wide.shape[1]), axis=0)

    def blocks_of(q, zz):
        return block(column(q // 2), lax.rem(c + q, 2), zz)

    def consume(zz, k, fresh):
        at = pl.ds(pl.multiple_of(k // layers * half, half), half)

        def step(q, carry):
            b = blocks_of(q, zz)

            @pl.when(fresh)
            def _():
                wait_chunk(b)

            @pl.when(lax.rem(q, 2) == 1)
            def _():
                for h in range(2):
                    wait_piece(b, k, h)

            compute(b, lax.rem(k, layers), at, slice(None))
            return carry

        lax.fori_loop(0, 2 * y_size, step, 0)

    total = last * count

    def z_duty(j):
        zz, k = plane(1 + j // count), lax.rem(j, count)
        onz = doubled(zz, k)

        @pl.when(middle | jnp.logical_not(onz))
        def _():
            duty(0, zz, k)

        @pl.when(middle & onz)
        def _():
            for o in range(1, y_size):
                duty(o, zz, k)

    lead = jnp.where(middle, count, 0)

    def ahead(j, carry):
        z_duty(j)
        return carry

    lax.fori_loop(0, lead, ahead, 0)

    def substep(m, carry):
        i, k = m // count, lax.rem(m, count)

        @pl.when(m + lead < total)
        def _():
            z_duty(m + lead)

        zz = plane(i)

        @pl.when((i == 0) | jnp.logical_not(doubled(zz, k)))
        def _():
            for o in range(1, y_size):
                duty(o, zz, k)

        consume(zz, k, k == 0)
        return carry

    lax.fori_loop(0, total, substep, 0)

    load_magnitude.wait()
    far = plane(last)
    for q in range(2 * y_size):
        wait_chunk(blocks_of(q, far))

    band = min(128, tokens)

    def gather(layer, first, end, halves):
        cols = pl.ds(halves[0] * width, len(halves) * width)

        def step(q, carry):
            b = blocks_of(q, far)

            @pl.when(lax.rem(q, 2) == 1)
            def _():
                for h in halves:
                    wait_piece(b, layer, h)
                    wait_piece(b, layers + layer, h)

            compute(b, layer, slice(None), cols)
            return carry

        lax.fori_loop(first, end, step, 0)

    def finish(layer, carry):
        @pl.when(jnp.logical_not(middle))
        def _():
            duty(0, far, layers + layer)

        gather(layer, 0, 2, (0, 1))

        for h in range(2):
            for o in range(1, y_size):
                duty(o, far, layer, (h,))

                @pl.when(jnp.logical_not(middle))
                def _(o=o):
                    duty(o, far, layers + layer, (h,))

            gather(layer, 2, 2 * y_size, (h,))
            cols = pl.ds(h * width, width)
            norm = jnp.sqrt(jnp.sum(squares[layer, :, cols], axis=0, keepdims=True) + epsilon)
            factor = mbuf[pl.ds(layer, 1), :][:, h * width:(h + 1) * width] / norm

            def scale(t, inner, cols=cols, factor=factor):
                at = pl.ds(pl.multiple_of(t * band, band), band)
                out_ref[layer, at, cols] = (acc[layer, at, cols] * factor).astype(out_ref.dtype)
                return inner

            lax.fori_loop(0, tokens // band, scale, 0)
        return carry

    lax.fori_loop(0, layers, finish, 0)

    def sent(amount, sem):
        ref = wbuf.at[pl.ds(0, amount), 0]
        remote(ref, sem, arrive.at[0], partner).wait_send()

    for n in range(rep_size):
        amount = (n + 1) * layers + (y_size - 1) * layers // 2

        if n < last:
            @pl.when(z == n)
            def _(amount=amount):
                sent(amount, zup)

            @pl.when(z == last - n)
            def _(amount=amount):
                sent(amount, zdown)

    for p in range(1, y_size):
        @pl.when(middle)
        def _(p=p):
            sent(rep_size * layers - 2 * layers // 2, ysend.at[p - 1])

        @pl.when(jnp.logical_not(middle))
        def _(p=p):
            sent(rep_size * layers - layers // 2, ysend.at[p - 1])

    whole = wbuf.at[pl.ds(0, y_size * rep_size)]
    remote(whole, csend, arrive.at[0], partner).wait_send()
    for o in range(1, tp_size):
        chunks = pbuf.at[pl.ds(0, len(own_chunks))]
        remote(chunks, psend.at[o - 1], arrive.at[0], partner).wait_send()


def local(sizes, prompts, frozen_projection_weight, lowrank_down_factor, lowrank_up_factor, magnitude):
    tp_size, dp_size, rep_size = sizes
    layers, rows, columns = frozen_projection_weight.shape
    rank = lowrank_down_factor.shape[2]
    tokens = prompts.shape[0]
    blocks = dp_size * rep_size
    y_size = dp_size // 2
    count = 2 * layers
    dma = pltpu.SemaphoreType.DMA
    return pl.pallas_call(
        functools.partial(kernel, sizes),
        out_shape=pltpu.VMEM((layers, tokens, columns), jnp.bfloat16),
        in_specs=[pl.BlockSpec(memory_space=pl.ANY)] * 5,
        out_specs=pl.BlockSpec(memory_space=pltpu.VMEM),
        scratch_shapes=[
            pltpu.VMEM((blocks, layers, rows, columns), jnp.bfloat16),
            pltpu.VMEM((blocks, tokens, rows), jnp.bfloat16),
            pltpu.VMEM((layers, rank, rows), jnp.bfloat16),
            pltpu.VMEM((layers, rank, columns), jnp.bfloat16),
            pltpu.VMEM((layers, columns), jnp.float32),
            pltpu.VMEM((layers, tokens, columns), jnp.float32),
            pltpu.VMEM((layers, 8, columns), jnp.float32),
            dma((blocks * count * 2,)),
            dma(()),
            dma(()),
            dma((max(1, y_size - 1),)),
            dma(()),
            dma((max(1, tp_size - 1),)),
            dma((blocks,)),
            dma((blocks // tp_size,)),
            dma((count,)),
            dma((3,)),
        ],
        compiler_params=pltpu.CompilerParams(
            collective_id=0, has_side_effects=True, vmem_limit_bytes=61_000_000
        ),
        cost_estimate=pl.CostEstimate(
            flops=2 * layers * tokens * columns * rows * blocks, bytes_accessed=2 * blocks * rows * columns,
            transcendentals=0,
        ),
    )(prompts, frozen_projection_weight, jnp.swapaxes(lowrank_down_factor, 1, 2), lowrank_up_factor, magnitude)


def solution(mesh):
    in_specs = (
        P(("dp", "rep"), "tp"),
        P(None, ("dp", "rep"), "tp"),
        P(None, ("dp", "rep"), None),
        P(None, None, "tp"),
        P(None, "tp"),
    )
    out_specs = P(None, ("dp", "rep"), "tp")
    sizes = tuple(mesh.shape[name] for name in ("tp", "dp", "rep"))
    return jax.shard_map(
        functools.partial(local, sizes), mesh=mesh, in_specs=in_specs, out_specs=out_specs, check_vma=False
    )
```
